512 devices in a mesh: grp: 8 (over z), seq: 32 (over x, y_hi, core), hd: 2 (over y_lo).
Axes of the slice: x: 4, y: 8 (y_hi: 4, y_lo: 2; y = y_hi * 2 + y_lo), z: 8, core: 2. Of those that a mesh axis runs over, the one named last changes fastest.
Arguments:
- latent_qkv: bfloat16 [8, 32, 256, 3, 3072], P('grp', 'seq', None, None, 'hd'), may hold values from -6 to 6
- cross_query: bfloat16 [8, 32, 256, 3072], P('grp', 'seq', None, 'hd'), may hold values from -6 to 6
- residual: bfloat16 [8, 32, 256, 3072], P('grp', 'seq', None, 'hd'), may hold values from -4 to 4
- prompt_states: bfloat16 [8, 512, 4096], P(None, 'seq', 'grp'), may hold values from -6 to 6
- kv_weight: bfloat16 [4096, 2, 3072], P(('grp', 'seq'), None, 'hd'), may hold values from -0.09375 to 0.09375, as said below
- prompt_lengths: int32 [8], replicated, may hold values from 32 to 512
- assignment: int32 [8], replicated, may hold values from 0 to 7, each once
Outputs:
- block_out: bfloat16 [8, 32, 256, 3072], P('grp', 'seq', None, 'hd')
The draws below stay inside these ranges and needn't reach their ends.
Inputs may be any that keep to these rules, and one draw needn't show every extreme that they name: Replica g serves prompt assignment[g]; every prompt is served by exactly one replica. `prompt_lengths`: key positions at or beyond a prompt's length are padding. `kv_weight`: entries have mean 0 and deviation 4096 ** -0.5.
All inputs are finite; a program needn't handle non-finite values.
Results may differ from the reference program's by a relative error of at most 0.0075.
Values may be sent and summed in bfloat16 or wider, within the bound.
A program may use at most 64 MiB of HBM per device.

```python
import math
import jax
import jax.numpy as jnp
from jax import lax

D = 4096
HEADS = 24
HDIM = 128
PLEN = 512
SPATIAL = 256
DM = 3072
FRAMES = 32
PROMPTS = 8
N_GRP = 8


def clipped_normal(sub_key, dims):
    return jnp.clip(jax.random.normal(sub_key, dims, jnp.float32), -6.0, 6.0)


def weight_table(key):
    bound_value = 6.0 / math.sqrt(D)
    sampled = jax.random.normal(jax.random.fold_in(key, 101), (D, 2, DM), jnp.float32) / math.sqrt(D)
    sampled = jnp.clip(sampled, -bound_value, bound_value)
    return sampled.astype(jnp.bfloat16).astype(jnp.float32)


def draw_kv_weight(key, part):
    return weight_table(key).astype(jnp.bfloat16)


def draw_prompt_states(key, part):
    full_shape = (PROMPTS, PLEN, D)
    sampled = clipped_normal(jax.random.fold_in(key, 1), full_shape)
    return sampled.astype(jnp.bfloat16)


def draw_cross_query(key, part):
    full_shape = (N_GRP, FRAMES, SPATIAL, DM)
    sampled = clipped_normal(jax.random.fold_in(key, 2), full_shape)
    return sampled.astype(jnp.bfloat16)


def draw_latent_qkv(key, part):
    full_shape = (N_GRP, FRAMES, SPATIAL, 3, DM)
    sampled = clipped_normal(jax.random.fold_in(key, 3), full_shape)
    return sampled.astype(jnp.bfloat16)


def set_ends(values, stream_key, low, top_value):
    index_at = [jax.random.randint(jax.random.fold_in(stream_key, axis), (), 0, length) for axis, length in enumerate(values.shape)]
    main_axis = values.shape.index(max(values.shape))
    next_to = index_at[:main_axis] + [(index_at[main_axis] + 1) % values.shape[main_axis]] + index_at[main_axis + 1:]
    return values.at[tuple(index_at)].set(low).at[tuple(next_to)].set(top_value)


def shard_levels(stream_key, shape, pieces, smallest, high):
    gain = 1.0
    for axis_at, shards_of in pieces:
        heights = jax.random.uniform(jax.random.fold_in(jax.random.fold_in(stream_key, 6), axis_at), (shards_of,), jnp.float32, smallest / len(pieces), high / len(pieces))
        gain = gain * jnp.repeat(jnp.exp(heights), shape[axis_at] // shards_of).reshape((-1,) + (1,) * (len(shape) - 1 - axis_at))
    return gain


def bell_draw(own_key, extent, scale, bound, shards=(), dtype=jnp.bfloat16):
    result = scale * jax.random.normal(own_key, extent, jnp.float32)
    if shards:
        result = result * shard_levels(own_key, extent, shards, -0.22, 0.18)
    return jnp.clip(result, -bound, bound).astype(dtype)


def setup_inputs(seed: int = 0) -> dict:
    key_list = jax.random.split(jax.random.key(seed), 8)
    latent_qkv = draw_latent_qkv(jax.random.fold_in(key_list[7], 71), 0)
    cross_query = draw_cross_query(jax.random.fold_in(key_list[7], 71), 0)
    residual = bell_draw(key_list[2], (N_GRP, FRAMES, SPATIAL, DM), 0.5, 4.0, ((0, 8), (1, 32), (3, 2)))
    prompt_states = draw_prompt_states(jax.random.fold_in(key_list[7], 71), 0)
    kv_weight = draw_kv_weight(jax.random.fold_in(key_list[7], 71), 0)
    prompt_lengths = set_ends(jax.random.randint(key_list[5], (PROMPTS,), max(1, PLEN // 16), PLEN + 1), jax.random.fold_in(key_list[5], 1), max(1, PLEN // 16), PLEN).astype(jnp.int32)
    assignment = jax.random.permutation(key_list[6], N_GRP).astype(jnp.int32)
    return dict(latent_qkv=latent_qkv, cross_query=cross_query, residual=residual, prompt_states=prompt_states, kv_weight=kv_weight, prompt_lengths=prompt_lengths, assignment=assignment)


def attend(queries, key_rows, values, key_bias):
    scores = jnp.einsum('qhe,khe->hqk', queries.astype(jnp.float32), key_rows.astype(jnp.float32))
    scores = scores / math.sqrt(queries.shape[-1]) + key_bias
    row_max = lax.optimization_barrier(jnp.max(scores, axis=-1, keepdims=True))
    powered = jnp.exp(scores - row_max)
    weights = (powered / lax.optimization_barrier(jnp.sum(powered, axis=-1, keepdims=True))).astype(jnp.bfloat16)
    return jnp.einsum('hqk,khe->qhe', weights.astype(jnp.float32), values.astype(jnp.float32))

def reference(latent_qkv, cross_query, residual, prompt_states, kv_weight, prompt_lengths, assignment):

    def one_group(group_index):
        chosen = assignment[group_index]
        prompt = prompt_states[chosen]
        pairs = jnp.dot(prompt, kv_weight.reshape(D, 2 * DM), preferred_element_type=jnp.float32)
        pairs = pairs.astype(jnp.bfloat16).reshape(PLEN, 2, HEADS, HDIM)
        key_bias = jnp.where(jnp.arange(PLEN) < prompt_lengths[chosen], 0.0, -1000000000.0).astype(jnp.float32)
        latent = latent_qkv[group_index].reshape(FRAMES, SPATIAL, 3, HEADS, HDIM)
        crossing = cross_query[group_index].reshape(FRAMES, SPATIAL, HEADS, HDIM)

        def one_frame(frame_index):
            local = latent[frame_index]
            spatial_out = attend(local[:, 0], local[:, 1], local[:, 2], jnp.float32(0.0))
            cross_out = attend(crossing[frame_index], pairs[:, 0], pairs[:, 1], key_bias)
            return spatial_out + cross_out
        framewise = lax.map(one_frame, jnp.arange(FRAMES))
        scores = jnp.einsum('fnhe,gnhe->nhfg', latent[:, :, 0].astype(jnp.float32), latent[:, :, 1].astype(jnp.float32))
        scores = scores / math.sqrt(HDIM)
        row_max = lax.optimization_barrier(jnp.max(scores, axis=-1, keepdims=True))
        powered = jnp.exp(scores - row_max)
        weights = (powered / lax.optimization_barrier(jnp.sum(powered, axis=-1, keepdims=True))).astype(jnp.bfloat16)
        temporal = jnp.einsum('nhfg,gnhe->fnhe', weights.astype(jnp.float32), latent[:, :, 2].astype(jnp.float32))
        temporal = temporal.astype(jnp.bfloat16).astype(jnp.float32)
        total = residual[group_index].astype(jnp.float32) + framewise.reshape(FRAMES, SPATIAL, DM)
        total = total + temporal.reshape(FRAMES, SPATIAL, DM)
        return total.astype(jnp.bfloat16)
    return lax.map(one_group, jnp.arange(N_GRP))
```

```python
import functools
import math

import jax
import jax.numpy as jnp
from jax import lax
from jax.experimental import pallas as pl
from jax.experimental.pallas import tpu as pltpu
from jax.sharding import PartitionSpec as P

HDIM = 128
SCALE = 1.0 / math.sqrt(HDIM)
MESH = pl.DeviceIdType.MESH
NX, NY, NC, NZ = 4, 4, 2, 8
ROWS = 16
FEAT = 512
CB = 768


def project_kernel(assign_ref, a_ref, w_ref, g_ref, ag, wg, part, got,
                   wx_s, wx_r, ar_s, ar_r, wr_s, wr_r, wc_s, wc_r, z_s, z_r,
                   gy_s, gy_r, gx_s, gx_r, gc_s, gc_r, loc_s):
    z = lax.axis_index("grp")
    s = lax.axis_index("seq")
    h = lax.axis_index("hd")
    x = s // 8
    y = (s // 2) % 4
    c = s % 2

    def dev(zz, xx, yy, cc):
        return (zz, (xx * 4 + yy) * 2 + cc, h)

    def put(src, dst, ss, rs, to):
        return pltpu.make_async_remote_copy(
            src_ref=src, dst_ref=dst, send_sem=ss, recv_sem=rs,
            device_id=to, device_id_type=MESH)

    barrier = pltpu.get_barrier_semaphore()
    peers = ([dev(z, (x + k) % 4, y, c) for k in (1, 2, 3)]
             + [dev(z, x, (y + k) % 4, c) for k in (1, 3)]
             + [dev(z, x, y, 1 - c)]
             + [dev((z + k) % 8, x, y, c) for k in range(1, 8)])
    for p in peers:
        pl.semaphore_signal(barrier, inc=1, device_id=p, device_id_type=MESH)
    pl.semaphore_wait(barrier, len(peers))

    def ring(me, at, lo, hi, to, ss, rs):
        left, right = (me + 3) % 4, (me + 1) % 4
        opp = (me + 2) % 4
        first = [put(at(me), at(me), ss.at[0], rs.at[0], to(right)),
                 put(at(me), at(me), ss.at[1], rs.at[1], to(left))]
        second = [put(lo(left), lo(left), ss.at[2], rs.at[2], to(right)),
                  put(hi(right), hi(right), ss.at[3], rs.at[3], to(left))]
        arrive = [put(at(left), at(left), ss.at[0], rs.at[0], to(right)),
                  put(at(right), at(right), ss.at[1], rs.at[1], to(left)),
                  put(lo(opp), lo(opp), ss.at[2], rs.at[2], to(right)),
                  put(hi(opp), hi(opp), ss.at[3], rs.at[3], to(left))]

        def start():
            first[0].start()
            first[1].start()

        def forward():
            arrive[0].wait_recv()
            second[0].start()
            arrive[1].wait_recv()
            second[1].start()

        def finish():
            arrive[2].wait_recv()
            arrive[3].wait_recv()
            for d in first + second:
                d.wait_send()

        return start, forward, finish

    own_w = pltpu.make_async_copy(w_ref.at[x], wg.at[x, y, c], loc_s.at[0])
    own_w.start()
    own_a = pltpu.make_async_copy(a_ref, ag.at[x], loc_s.at[1])
    own_a.start()
    wx = []
    for k in (1, 2, 3):
        to = (x + k) % 4
        d = put(w_ref.at[to], wg.at[x, y, c], wx_s.at[k - 1], wx_r.at[k - 1], dev(z, to, y, c))
        d.start()
        wx.append(d)
    own_a.wait()
    a_start, a_forward, a_finish = ring(
        x, lambda k: ag.at[k], lambda k: ag.at[k, 0:4], lambda k: ag.at[k, 4:8],
        lambda k: dev(z, k, y, c), ar_s, ar_r)
    a_start()
    own_w.wait()
    for k in (1, 2, 3):
        frm = (x + 4 - k) % 4
        put(w_ref.at[x], wg.at[frm, y, c], wx_s.at[k - 1], wx_r.at[k - 1],
            dev(z, frm, y, c)).wait_recv()
    w_start, w_forward, w_finish = ring(
        y, lambda k: wg.at[:, k, c], lambda k: wg.at[0:2, k, c], lambda k: wg.at[2:4, k, c],
        lambda k: dev(z, x, k, c), wr_s, wr_r)
    w_start()
    a_forward()
    w_forward()
    a_finish()
    w_finish()
    swap = put(wg.at[:, :, c], wg.at[:, :, c], wc_s, wc_r, dev(z, x, y, 1 - c))
    swap.start()
    put(wg.at[:, :, 1 - c], wg.at[:, :, 1 - c], wc_s, wc_r, dev(z, x, y, 1 - c)).wait_recv()

    for half in range(2):
        lhs = jnp.concatenate(
            [ag[xb, assign_ref[half * 4 + j]] for j in range(4) for xb in range(4)], axis=0)
        rhs = wg[...].reshape(FEAT, CB)
        prod = jnp.dot(lhs, rhs, preferred_element_type=jnp.float32)
        part[half * 4:half * 4 + 4] = prod.astype(jnp.bfloat16).reshape(4, 64, CB)
    sent = []
    for k in (4, 3, 5, 2, 6, 1, 7):
        to = (z + k) % 8
        d = put(part.at[to], got.at[k - 1], z_s.at[k - 1], z_r.at[k - 1], dev(to, x, y, c))
        d.start()
        sent.append(d)
    for d in wx:
        d.wait_send()
    swap.wait_send()
    total = part[z].astype(jnp.float32)
    for k in range(1, 8):
        frm = (z + 8 - k) % 8
        put(part.at[0], got.at[k - 1], z_s.at[k - 1], z_r.at[k - 1], dev(frm, x, y, c)).wait_recv()
        total = total + got[k - 1].astype(jnp.float32)
    g_ref[x, y, c] = total.astype(jnp.bfloat16)

    y_start, y_forward, y_finish = ring(
        y, lambda k: g_ref.at[x, k, c], lambda k: g_ref.at[x, k, c, 0:32],
        lambda k: g_ref.at[x, k, c, 32:64], lambda k: dev(z, x, k, c), gy_s, gy_r)
    y_start()
    y_forward()
    y_finish()
    x_start, x_forward, x_finish = ring(
        x, lambda k: g_ref.at[k, :, c], lambda k: g_ref.at[k, 0:2, c],
        lambda k: g_ref.at[k, 2:4, c], lambda k: dev(z, k, y, c), gx_s, gx_r)

    def to_core(k, i):
        return put(g_ref.at[k, :, c], g_ref.at[k, :, c], gc_s.at[i], gc_r.at[i], dev(z, x, y, 1 - c))

    x_start()
    swaps = [to_core((x + k) % 4, i) for i, k in enumerate((0, 3, 1, 2))]
    swaps[0].start()
    x_forward()
    swaps[1].start()
    swaps[2].start()
    x_finish()
    swaps[3].start()
    for d in sent:
        d.wait_send()
    for i, k in enumerate((0, 3, 1, 2)):
        b = (x + k) % 4
        put(g_ref.at[b, :, 1 - c], g_ref.at[b, :, 1 - c], gc_s.at[i], gc_r.at[i],
            dev(z, x, y, 1 - c)).wait_recv()
    for d in swaps:
        d.wait_send()


def project(assignment, prompts, weight):
    sem = pltpu.SemaphoreType.DMA
    vm = pl.BlockSpec(memory_space=pltpu.VMEM)
    return pl.pallas_call(
        project_kernel,
        out_shape=jax.ShapeDtypeStruct((NX, NY, NC, 64, CB), jnp.bfloat16),
        in_specs=[pl.BlockSpec(memory_space=pltpu.SMEM), vm, vm],
        out_specs=vm,
        scratch_shapes=[
            pltpu.VMEM((NX, 8, ROWS, FEAT), jnp.bfloat16),
            pltpu.VMEM((NX, NY, NC, ROWS, CB), jnp.bfloat16),
            pltpu.VMEM((NZ, 64, CB), jnp.bfloat16),
            pltpu.VMEM((NZ - 1, 64, CB), jnp.bfloat16),
            sem((3,)), sem((3,)), sem((4,)), sem((4,)), sem((4,)), sem((4,)),
            sem, sem, sem((7,)), sem((7,)),
            sem((4,)), sem((4,)), sem((4,)), sem((4,)), sem((4,)), sem((4,)), sem((2,)),
        ],
        compiler_params=pltpu.CompilerParams(
            collective_id=0, has_side_effects=True, vmem_limit_bytes=24 * 2**20),
        cost_estimate=pl.CostEstimate(flops=2 * 10**8, bytes_accessed=8 * 10**6, transcendentals=0),
        name="project",
    )(assignment, prompts, weight)


def soft(scores):
    top = jnp.max(scores, axis=-1, keepdims=True)
    powered = jnp.exp(scores - top)
    return (powered * (1.0 / jnp.sum(powered, axis=-1, keepdims=True))).astype(jnp.bfloat16)


def qk(q, k):
    return lax.dot_general(q, k, (((1,), (1,)), ((), ())), preferred_element_type=jnp.float32) * SCALE


def spatial_kernel(lat_ref, res_ref, out_ref):
    for i in range(2):
        cols = slice(i * HDIM, (i + 1) * HDIM)
        w = soft(qk(lat_ref[0, :, cols], lat_ref[1, :, cols]))
        o = jnp.dot(w, lat_ref[2, :, cols], preferred_element_type=jnp.float32)
        out_ref[:, cols] = res_ref[:, cols].astype(jnp.float32) + o


def spatial_part(latent, residual):
    wide = 2 * HDIM
    return pl.pallas_call(
        spatial_kernel,
        out_shape=jax.ShapeDtypeStruct(residual.shape, jnp.float32),
        grid=(residual.shape[1] // wide,),
        in_specs=[pl.BlockSpec((3, 256, wide), lambda i: (0, 0, i)),
                  pl.BlockSpec((256, wide), lambda i: (0, i))],
        out_specs=pl.BlockSpec((256, wide), lambda i: (0, i)),
        cost_estimate=pl.CostEstimate(flops=10**7, bytes_accessed=5 * 10**6, transcendentals=10**6),
        name="spatial",
    )(latent, residual)


def temporal_kernel(in_ref, out_ref):
    row = lax.broadcasted_iota(jnp.int32, (256, 256), 0) % 8
    col = lax.broadcasted_iota(jnp.int32, (256, 256), 1) % 8
    for i in range(2):
        cols = slice(i * HDIM, (i + 1) * HDIM)
        q, k, v = (in_ref[:, j, :, cols].reshape(256, HDIM) for j in range(3))
        w = soft(jnp.where(row == col, qk(q, k), -1e30))
        o = jnp.dot(w, v, preferred_element_type=jnp.float32)
        out_ref[:, :, cols] = o.astype(jnp.bfloat16).reshape(32, 8, HDIM)


def temporal_part(moved):
    wide = 2 * HDIM
    return pl.pallas_call(
        temporal_kernel,
        out_shape=jax.ShapeDtypeStruct((32, 8, moved.shape[3]), jnp.bfloat16),
        grid=(moved.shape[3] // wide,),
        in_specs=[pl.BlockSpec((32, 3, 8, wide), lambda i: (0, 0, 0, i))],
        out_specs=pl.BlockSpec((32, 8, wide), lambda i: (0, 0, i)),
        cost_estimate=pl.CostEstimate(flops=10**7, bytes_accessed=5 * 10**6, transcendentals=10**6),
        name="temporal",
    )(moved)


def cross_kernel(len_ref, q_ref, k_ref, v_ref, acc_ref, out_ref):
    r = lax.broadcasted_iota(jnp.int32, (1, 512), 1)
    yy, cc, xb, i = r // 128, (r // 64) % 2, (r // 16) % 4, r % 16
    pos = ((xb * 4 + yy) * 2 + cc) * 16 + i
    bias = jnp.where(pos < len_ref[0], 0.0, -1e9)
    for i in range(2):
        cols = slice(i * HDIM, (i + 1) * HDIM)
        w = soft(qk(q_ref[:, cols], k_ref[0, :, cols]) + bias)
        o = jnp.dot(w, v_ref[0, :, cols], preferred_element_type=jnp.float32)
        out_ref[:, cols] = acc_ref[:, cols] + o


def cross_part(length, query, pairs, acc):
    wide = 2 * HDIM
    return pl.pallas_call(
        cross_kernel,
        out_shape=jax.ShapeDtypeStruct(acc.shape, jnp.float32),
        grid=(acc.shape[1] // wide,),
        in_specs=[pl.BlockSpec(memory_space=pltpu.SMEM),
                  pl.BlockSpec((256, wide), lambda i: (0, i)),
                  pl.BlockSpec((1, 512, wide), lambda i: (i // 3, 0, i % 3)),
                  pl.BlockSpec((1, 512, wide), lambda i: (2 + i // 3, 0, i % 3)),
                  pl.BlockSpec((256, wide), lambda i: (0, i))],
        out_specs=pl.BlockSpec((256, wide), lambda i: (0, i)),
        cost_estimate=pl.CostEstimate(flops=10**7, bytes_accessed=8 * 10**6, transcendentals=10**6),
        name="cross",
    )(length, query, pairs, pairs, acc)


def body(latent_qkv, cross_query, residual, prompt_states, kv_weight, prompt_lengths, assignment):
    latent = jnp.transpose(latent_qkv[0, 0], (1, 0, 2))
    blocked = jnp.transpose(latent.reshape(3, 32, 8, 1536), (1, 0, 2, 3))
    moved = lax.all_to_all(blocked, "seq", split_axis=0, concat_axis=0, tiled=True)
    weight = jnp.transpose(kv_weight.reshape(ROWS, 4, CB), (1, 0, 2))
    pairs = project(assignment, prompt_states, weight)
    acc = spatial_part(latent, residual[0, 0])
    moved, pairs, acc = lax.optimization_barrier((moved, pairs, acc))
    returned = lax.all_to_all(temporal_part(moved), "seq", split_axis=0, concat_axis=0, tiled=True)
    served = assignment[lax.axis_index("grp")]
    length = lax.dynamic_slice(prompt_lengths, (served,), (1,))
    acc = cross_part(length, cross_query[0, 0], pairs.reshape(4, 512, CB), acc)
    total = acc + returned.reshape(256, 1536).astype(jnp.float32)
    return total.astype(jnp.bfloat16)[None, None]


def solution(mesh):
    return jax.shard_map(
        body,
        mesh=mesh,
        in_specs=(
            P("grp", "seq", None, None, "hd"),
            P("grp", "seq", None, "hd"),
            P("grp", "seq", None, "hd"),
            P(None, "seq", "grp"),
            P(("grp", "seq"), None, "hd"),
            P(),
            P(),
        ),
        out_specs=P("grp", "seq", None, "hd"),
        check_vma=False,
    )
```

```python
import math

import jax
import jax.numpy as jnp
from jax import lax
from jax.experimental import pallas as pl
from jax.experimental.pallas import tpu as pltpu
from jax.sharding import PartitionSpec as P

HDIM = 128
SCALE = 1.0 / math.sqrt(HDIM)
MESH = pl.DeviceIdType.MESH
ROWS, FEAT, CB, HALF = 16, 512, 768, 768


def soft(scores):
    top = jnp.max(scores, axis=-1, keepdims=True)
    powered = jnp.exp(scores - top)
    return (powered * (1.0 / jnp.sum(powered, axis=-1, keepdims=True))).astype(jnp.bfloat16)


def qk(q, k):
    return lax.dot_general(q, k, (((1,), (1,)), ((), ())), preferred_element_type=jnp.float32) * SCALE


def lanes(i):
    return pl.ds(pl.multiple_of(i * HDIM, HDIM), HDIM)


def block_kernel(assign_ref, len_ref, lat_ref, cq_ref, res_ref, a_ref, w_ref, out_ref,
                 lat, cq, res, acc, mv0, mv1, t0, t1, rt0, rt1, ag, wg, part, got, g,
                 loc, ex_s, ex_r, rt_s, rt_r,
                 wx_s, wx_r, ar_s, ar_r, wr_s, wr_r, wc_s, wc_r, z_s, z_r,
                 gy_s, gy_r, gx_s, gx_r, gc_s, gc_r):
    z = lax.axis_index("grp")
    s = lax.axis_index("seq")
    h = lax.axis_index("hd")
    x = s // 8
    y = (s // 2) % 4
    c = s % 2

    def dev(zz, xx, yy, cc):
        return (zz, (xx * 4 + yy) * 2 + cc, h)

    def put(src, dst, ss, rs, to):
        return pltpu.make_async_remote_copy(
            src_ref=src, dst_ref=dst, send_sem=ss, recv_sem=rs,
            device_id=to, device_id_type=MESH)

    def peer(t):
        return (((x + t // 8) % 4) * 4 + (y + t) % 4) * 2 + (c + t // 4) % 2

    mvs, ts, rts = (mv0, mv1), (t0, t1), (rt0, rt1)
    cols = (pl.ds(0, HALF), pl.ds(HALF, HALF))
    local = [
        pltpu.make_async_copy(w_ref.at[x], wg.at[x, y, c], loc.at[0]),
        pltpu.make_async_copy(a_ref, ag.at[x], loc.at[1]),
        pltpu.make_async_copy(lat_ref, lat, loc.at[2]),
        pltpu.make_async_copy(res_ref, res, loc.at[3]),
        pltpu.make_async_copy(lat_ref.at[:, s, :, cols[0]], mv0.at[s], loc.at[4]),
        pltpu.make_async_copy(lat_ref.at[:, s, :, cols[1]], mv1.at[s], loc.at[5]),
        pltpu.make_async_copy(cq_ref, cq, loc.at[6]),
    ]
    for d in local:
        d.start()

    barrier = pltpu.get_barrier_semaphore()

    @pl.loop(1, 32)
    def _(t):
        pl.semaphore_signal(barrier, inc=1, device_id=(z, peer(t), h), device_id_type=MESH)

    @pl.loop(1, 8)
    def _(k):
        pl.semaphore_signal(barrier, inc=1, device_id=((z + k) % 8, s, h), device_id_type=MESH)

    pl.semaphore_wait(barrier, 38)

    def ring(me, at, lo, hi, to, ss, rs):
        left, right = (me + 3) % 4, (me + 1) % 4
        opp = (me + 2) % 4
        first = [put(at(me), at(me), ss.at[0], rs.at[0], to(right)),
                 put(at(me), at(me), ss.at[1], rs.at[1], to(left))]
        second = [put(lo(left), lo(left), ss.at[2], rs.at[2], to(right)),
                  put(hi(right), hi(right), ss.at[3], rs.at[3], to(left))]
        arrive = [put(at(left), at(left), ss.at[0], rs.at[0], to(right)),
                  put(at(right), at(right), ss.at[1], rs.at[1], to(left)),
                  put(lo(opp), lo(opp), ss.at[2], rs.at[2], to(right)),
                  put(hi(opp), hi(opp), ss.at[3], rs.at[3], to(left))]

        def start():
            first[0].start()
            first[1].start()

        def forward():
            arrive[0].wait_recv()
            second[0].start()
            arrive[1].wait_recv()
            second[1].start()

        def finish():
            arrive[2].wait_recv()
            arrive[3].wait_recv()

        def drain():
            for d in first + second:
                d.wait_send()

        return start, forward, finish, drain

    def exchange(half, lo, hi):
        @pl.loop(lo, hi)
        def _(t):
            to = peer(t)
            put(lat_ref.at[:, to, :, cols[half]], mvs[half].at[s],
                ex_s.at[half], ex_r.at[half], (z, to, h)).start()

    def give_back(half):
        @pl.loop(1, 32)
        def _(t):
            to = peer(t)
            put(ts[half].at[to], rts[half].at[s], rt_s.at[half], rt_r.at[half], (z, to, h)).start()

    def all_of(ref, ss, rs, half):
        whole = ref.at[pl.ds(0, 31)]
        return put(whole, whole, ss.at[half], rs.at[half], (z, peer(1), h))

    def spatial(lo, hi):
        @pl.loop(lo, hi)
        def _(i):
            for j in range(2):
                at = lanes(i * 2 + j)
                q, k, v = (lat[n, :, :, at].reshape(256, HDIM) for n in range(3))
                o = jnp.dot(soft(qk(q, k)), v, preferred_element_type=jnp.float32)
                acc[:, at] = res[:, at].astype(jnp.float32) + o

    def temporal(half):
        mv, t = mvs[half], ts[half]
        row = lax.broadcasted_iota(jnp.int32, (256, 256), 0) % 8
        col = lax.broadcasted_iota(jnp.int32, (256, 256), 1) % 8

        @pl.loop(0, 3)
        def _(i):
            for j in range(2):
                at = lanes(i * 2 + j)
                q, k, v = (mv[:, n, :, at].reshape(256, HDIM) for n in range(3))
                w = soft(jnp.where(row == col, qk(q, k), -1e30))
                o = jnp.dot(w, v, preferred_element_type=jnp.float32)
                t[:, :, at] = o.astype(jnp.bfloat16).reshape(32, 8, HDIM)

        rts[half][pl.ds(s, 1)] = t[pl.ds(s, 1)]

    r = lax.broadcasted_iota(jnp.int32, (1, 512), 1)
    pos = ((((r // 16) % 4) * 4 + r // 128) * 2 + (r // 64) % 2) * 16 + r % 16
    bias = jnp.where(pos < len_ref[assign_ref[z]], 0.0, -1e9)

    def cross(b):
        for j in range(3):
            at = lanes(b * 3 + j)
            k = g[b, :, :, :, j * HDIM:(j + 1) * HDIM].reshape(512, HDIM)
            v = g[b, :, :, :, 384 + j * HDIM:384 + (j + 1) * HDIM].reshape(512, HDIM)
            w = soft(qk(cq[:, at], k) + bias)
            acc[:, at] = acc[:, at] + jnp.dot(w, v, preferred_element_type=jnp.float32)

    wx = []
    for k in (1, 2, 3):
        to = (x + k) % 4
        d = put(w_ref.at[to], wg.at[x, y, c], wx_s.at[k - 1], wx_r.at[k - 1], dev(z, to, y, c))
        d.start()
        wx.append(d)
    local[1].wait()
    a_start, a_forward, a_finish, a_drain = ring(
        x, lambda k: ag.at[k], lambda k: ag.at[k, 0:4], lambda k: ag.at[k, 4:8],
        lambda k: dev(z, k, y, c), ar_s, ar_r)
    a_start()
    exchange(0, 1, 8)
    local[0].wait()
    for k in (1, 2, 3):
        frm = (x + 4 - k) % 4
        put(w_ref.at[x], wg.at[frm, y, c], wx_s.at[k - 1], wx_r.at[k - 1],
            dev(z, frm, y, c)).wait_recv()
    w_start, w_forward, w_finish, w_drain = ring(
        y, lambda k: wg.at[:, k, c], lambda k: wg.at[0:2, k, c], lambda k: wg.at[2:4, k, c],
        lambda k: dev(z, x, k, c), wr_s, wr_r)
    w_start()
    exchange(0, 8, 16)
    local[2].wait()
    local[3].wait()
    spatial(0, 2)
    a_forward()
    w_forward()
    exchange(0, 16, 32)
    exchange(1, 1, 8)
    spatial(2, 6)
    a_finish()
    w_finish()
    swap = put(wg.at[:, :, c], wg.at[:, :, c], wc_s, wc_r, dev(z, x, y, 1 - c))
    swap.start()
    put(wg.at[:, :, 1 - c], wg.at[:, :, 1 - c], wc_s, wc_r, dev(z, x, y, 1 - c)).wait_recv()

    for half in range(2):
        lhs = jnp.concatenate(
            [ag[xb, assign_ref[half * 4 + j]] for j in range(4) for xb in range(4)], axis=0)
        prod = jnp.dot(lhs, wg[...].reshape(FEAT, CB), preferred_element_type=jnp.float32)
        part[half * 4:half * 4 + 4] = prod.astype(jnp.bfloat16).reshape(4, 64, CB)
    sent = []
    for k in (4, 3, 5, 2, 6, 1, 7):
        to = (z + k) % 8
        d = put(part.at[to], got.at[k - 1], z_s.at[k - 1], z_r.at[k - 1], dev(to, x, y, c))
        d.start()
        sent.append(d)

    exchange(1, 8, 20)
    all_of(mv0, ex_s, ex_r, 0).wait_recv()
    local[4].wait()
    temporal(0)

    total = part[z].astype(jnp.float32)
    for k in range(1, 8):
        frm = (z + 8 - k) % 8
        put(part.at[0], got.at[k - 1], z_s.at[k - 1], z_r.at[k - 1], dev(frm, x, y, c)).wait_recv()
        total = total + got[k - 1].astype(jnp.float32)
    g[x, y, c] = total.astype(jnp.bfloat16)

    y_start, y_forward, y_finish, y_drain = ring(
        y, lambda k: g.at[x, k, c], lambda k: g.at[x, k, c, 0:32],
        lambda k: g.at[x, k, c, 32:64], lambda k: dev(z, x, k, c), gy_s, gy_r)
    x_start, x_forward, x_finish, x_drain = ring(
        x, lambda k: g.at[k, :, c], lambda k: g.at[k, 0:2, c],
        lambda k: g.at[k, 2:4, c], lambda k: dev(z, k, y, c), gx_s, gx_r)
    blocks = [(x + k) % 4 for k in (0, 3, 1, 2)]
    swaps = [put(g.at[b, :, c], g.at[b, :, c], gc_s.at[i], gc_r.at[i], dev(z, x, y, 1 - c))
             for i, b in enumerate(blocks)]
    swapped = [put(g.at[b, :, 1 - c], g.at[b, :, 1 - c], gc_s.at[i], gc_r.at[i],
                   dev(z, x, y, 1 - c)) for i, b in enumerate(blocks)]
    y_start()
    exchange(1, 20, 32)
    y_forward()
    give_back(0)
    y_finish()
    x_start()
    swaps[0].start()
    local[6].wait()
    swapped[0].wait_recv()
    cross(blocks[0])

    all_of(mv1, ex_s, ex_r, 1).wait_recv()
    local[5].wait()
    temporal(1)
    give_back(1)

    x_forward()
    swaps[1].start()
    swaps[2].start()
    swapped[1].wait_recv()
    cross(blocks[1])
    swapped[2].wait_recv()
    cross(blocks[2])
    x_finish()
    swaps[3].start()
    swapped[3].wait_recv()
    cross(blocks[3])

    for half in range(2):
        all_of(rts[half], rt_s, rt_r, half).wait_recv()
        back = rts[half][...].reshape(256, HALF).astype(jnp.float32)
        out_ref[:, cols[half]] = (acc[:, cols[half]] + back).astype(jnp.bfloat16)

    for half in range(2):
        all_of(mvs[half], ex_s, ex_r, half).wait_send()
        all_of(ts[half], rt_s, rt_r, half).wait_send()
    for d in wx + [swap] + sent + swaps:
        d.wait_send()
    a_drain()
    w_drain()
    y_drain()
    x_drain()


def body(latent_qkv, cross_query, residual, prompt_states, kv_weight, prompt_lengths, assignment):
    latent = jnp.transpose(latent_qkv[0, 0], (1, 0, 2)).reshape(3, 32, 8, 1536)
    weight = jnp.transpose(kv_weight.reshape(ROWS, 2, 4, 384), (2, 0, 1, 3)).reshape(4, ROWS, CB)
    sem = pltpu.SemaphoreType.DMA
    vm = pl.BlockSpec(memory_space=pltpu.VMEM)
    sm = pl.BlockSpec(memory_space=pltpu.SMEM)
    hb = pl.BlockSpec(memory_space=pl.ANY)
    b16, f32 = jnp.bfloat16, jnp.float32
    out = pl.pallas_call(
        block_kernel,
        out_shape=jax.ShapeDtypeStruct((256, 1536), b16),
        in_specs=[sm, sm, hb, hb, hb, vm, vm],
        out_specs=vm,
        scratch_shapes=[
            pltpu.VMEM((3, 32, 8, 1536), b16),
            pltpu.VMEM((256, 1536), b16),
            pltpu.VMEM((256, 1536), b16),
            pltpu.VMEM((256, 1536), f32),
            pltpu.VMEM((32, 3, 8, HALF), b16), pltpu.VMEM((32, 3, 8, HALF), b16),
            pltpu.VMEM((32, 8, HALF), b16), pltpu.VMEM((32, 8, HALF), b16),
            pltpu.VMEM((32, 8, HALF), b16), pltpu.VMEM((32, 8, HALF), b16),
            pltpu.VMEM((4, 8, ROWS, FEAT), b16),
            pltpu.VMEM((4, 4, 2, ROWS, CB), b16),
            pltpu.VMEM((8, 64, CB), b16),
            pltpu.VMEM((7, 64, CB), b16),
            pltpu.VMEM((4, 4, 2, 64, CB), b16),
            sem((7,)), sem((2,)), sem((2,)), sem((2,)), sem((2,)),
            sem((3,)), sem((3,)), sem((4,)), sem((4,)), sem((4,)), sem((4,)),
            sem, sem, sem((7,)), sem((7,)),
            sem((4,)), sem((4,)), sem((4,)), sem((4,)), sem((4,)), sem((4,)),
        ],
        compiler_params=pltpu.CompilerParams(collective_id=0, has_side_effects=True),
        name="block",
    )(assignment, prompt_lengths, latent, cross_query[0, 0], residual[0, 0], prompt_states, weight)
    return out[None, None]


def solution(mesh):
    return jax.shard_map(
        body,
        mesh=mesh,
        in_specs=(
            P("grp", "seq", None, None, "hd"),
            P("grp", "seq", None, "hd"),
            P("grp", "seq", None, "hd"),
            P(None, "seq", "grp"),
            P(("grp", "seq"), None, "hd"),
            P(),
            P(),
        ),
        out_specs=P("grp", "seq", None, "hd"),
        check_vma=False,
    )
```

```python
import math

import jax
import jax.numpy as jnp
from jax import lax
from jax.experimental import pallas as pl
from jax.experimental.pallas import tpu as pltpu
from jax.sharding import PartitionSpec as P

HDIM = 128
SCALE = 1.0 / math.sqrt(HDIM)
MESH = pl.DeviceIdType.MESH
ROWS, FEAT, CB, HALF = 16, 512, 768, 768


def soft(scores):
    top = jnp.max(scores, axis=-1, keepdims=True)
    powered = jnp.exp(scores - top)
    return (powered * (1.0 / jnp.sum(powered, axis=-1, keepdims=True))).astype(jnp.bfloat16)


def qk(q, k):
    return lax.dot_general(q, k, (((1,), (1,)), ((), ())), preferred_element_type=jnp.float32) * SCALE


def lanes(i):
    return pl.ds(pl.multiple_of(i * HDIM, HDIM), HDIM)


def block_kernel(assign_ref, len_ref, lat_ref, cq_ref, res_ref, a_ref, raw_ref, out_ref,
                 w_ref, lat, cq, res, acc, mv0, mv1, t0, t1, rt0, rt1, ag, wg, part0, part1, got0, got1, g0, g1,
                 loc, ex_s, ex_r, rt_s, rt_r,
                 wx_s, wx_r, ar_s, ar_r, wr_s, wr_r, wc_s, wc_r, z_s, z_r,
                 gy_s, gy_r, gx_s, gx_r, gc_s, gc_r):
    z = lax.axis_index("grp")
    s = lax.axis_index("seq")
    h = lax.axis_index("hd")
    x = s // 8
    y = (s // 2) % 4
    c = s % 2

    def dev(zz, xx, yy, cc):
        return (zz, (xx * 4 + yy) * 2 + cc, h)

    def put(src, dst, ss, rs, to):
        return pltpu.make_async_remote_copy(
            src_ref=src, dst_ref=dst, send_sem=ss, recv_sem=rs,
            device_id=to, device_id_type=MESH)

    def peer(t):
        return (((x + t // 8) % 4) * 4 + (y + t) % 4) * 2 + (c + t // 4) % 2

    mvs, ts, rts = (mv0, mv1), (t0, t1), (rt0, rt1)
    cols = (pl.ds(0, HALF), pl.ds(HALF, HALF))
    local = [
        pltpu.make_async_copy(a_ref, ag.at[x], loc.at[1]),
        pltpu.make_async_copy(lat_ref, lat, loc.at[2]),
        pltpu.make_async_copy(res_ref, res, loc.at[3]),
        pltpu.make_async_copy(lat_ref.at[:, s, :, cols[0]], mv0.at[s], loc.at[4]),
        pltpu.make_async_copy(lat_ref.at[:, s, :, cols[1]], mv1.at[s], loc.at[5]),
        pltpu.make_async_copy(cq_ref, cq, loc.at[6]),
    ]
    for d in local:
        d.start()

    barrier = pltpu.get_barrier_semaphore()

    @pl.loop(1, 32)
    def _(t):
        pl.semaphore_signal(barrier, inc=1, device_id=(z, peer(t), h), device_id_type=MESH)

    @pl.loop(1, 8)
    def _(k):
        pl.semaphore_signal(barrier, inc=1, device_id=((z + k) % 8, s, h), device_id_type=MESH)

    for n in range(2):
        rows = raw_ref[:, n, :]
        for k in range(4):
            w_ref[k, :, n * 384:(n + 1) * 384] = rows[:, k * 384:(k + 1) * 384]
    wg[x, y, c] = w_ref[x]
    pl.semaphore_wait(barrier, 38)

    def ring(me, at, lo, hi, to, ss, rs):
        left, right = (me + 3) % 4, (me + 1) % 4
        opp = (me + 2) % 4
        first = [put(at(me), at(me), ss.at[0], rs.at[0], to(right)),
                 put(at(me), at(me), ss.at[1], rs.at[1], to(left))]
        second = [put(lo(left), lo(left), ss.at[2], rs.at[2], to(right)),
                  put(hi(right), hi(right), ss.at[3], rs.at[3], to(left))]
        arrive = [put(at(left), at(left), ss.at[0], rs.at[0], to(right)),
                  put(at(right), at(right), ss.at[1], rs.at[1], to(left)),
                  put(lo(opp), lo(opp), ss.at[2], rs.at[2], to(right)),
                  put(hi(opp), hi(opp), ss.at[3], rs.at[3], to(left))]

        def start():
            first[0].start()
            first[1].start()

        def forward():
            arrive[0].wait_recv()
            second[0].start()
            arrive[1].wait_recv()
            second[1].start()

        def finish():
            arrive[2].wait_recv()
            arrive[3].wait_recv()

        def drain():
            for d in first + second:
                d.wait_send()

        return start, forward, finish, drain

    def exchange(half, lo, hi):
        @pl.loop(lo, hi)
        def _(t):
            to = peer(t)
            put(lat_ref.at[:, to, :, cols[half]], mvs[half].at[s],
                ex_s.at[half], ex_r.at[half], (z, to, h)).start()

    def give_back(half):
        @pl.loop(1, 32)
        def _(t):
            to = peer(t)
            put(ts[half].at[to], rts[half].at[s], rt_s.at[half], rt_r.at[half], (z, to, h)).start()

    def all_of(ref, ss, rs, half):
        whole = ref.at[pl.ds(0, 31)]
        return put(whole, whole, ss.at[half], rs.at[half], (z, peer(1), h))

    def spatial(lo, hi):
        @pl.loop(lo, hi)
        def _(i):
            for j in range(2):
                at = lanes(i * 2 + j)
                q, k, v = (lat[n, :, :, at].reshape(256, HDIM) for n in range(3))
                o = jnp.dot(soft(qk(q, k)), v, preferred_element_type=jnp.float32)
                acc[:, at] = res[:, at].astype(jnp.float32) + o

    def temporal(half):
        mv, t = mvs[half], ts[half]
        row = lax.broadcasted_iota(jnp.int32, (256, 256), 0) % 8
        col = lax.broadcasted_iota(jnp.int32, (256, 256), 1) % 8

        @pl.loop(0, 3)
        def _(i):
            for j in range(2):
                at = lanes(i * 2 + j)
                q, k, v = (mv[:, n, :, at].reshape(256, HDIM) for n in range(3))
                w = soft(jnp.where(row == col, qk(q, k), -1e30))
                o = jnp.dot(w, v, preferred_element_type=jnp.float32)
                t[:, :, at] = o.astype(jnp.bfloat16).reshape(32, 8, HDIM)

        rts[half][pl.ds(s, 1)] = t[pl.ds(s, 1)]

    r = lax.broadcasted_iota(jnp.int32, (1, 512), 1)
    pos = ((((r // 16) % 4) * 4 + r // 128) * 2 + (r // 64) % 2) * 16 + r % 16
    bias = jnp.where(pos < len_ref[assign_ref[z]], 0.0, -1e9)

    parts, gots, gs = (part0, part1), (got0, got1), (g0, g1)
    group_heads = ((0, 1), (2,))

    def cross(b, n):
        heads = group_heads[n]
        for j, head in enumerate(heads):
            at = lanes(b * 3 + head)
            vj = len(heads) + j
            k = gs[n][b, :, :, :, j * HDIM:(j + 1) * HDIM].reshape(512, HDIM)
            v = gs[n][b, :, :, :, vj * HDIM:(vj + 1) * HDIM].reshape(512, HDIM)
            w = soft(qk(cq[:, at], k) + bias)
            acc[:, at] = acc[:, at] + jnp.dot(w, v, preferred_element_type=jnp.float32)

    wx = [put(w_ref.at[(x + k) % 4], wg.at[x, y, c], wx_s.at[k - 1], wx_r.at[k - 1],
              dev(z, (x + k) % 4, y, c)) for k in (1, 2, 3)]
    wx_in = [put(w_ref.at[x], wg.at[(x + 4 - k) % 4, y, c], wx_s.at[k - 1], wx_r.at[k - 1],
                 dev(z, (x + 4 - k) % 4, y, c)) for k in (1, 2, 3)]
    a_start, a_forward, a_finish, a_drain = ring(
        x, lambda k: ag.at[k], lambda k: ag.at[k, 0:4], lambda k: ag.at[k, 4:8],
        lambda k: dev(z, k, y, c), ar_s, ar_r)
    w_start, w_forward, w_finish, w_drain = ring(
        y, lambda k: wg.at[:, k, c], lambda k: wg.at[0:2, k, c], lambda k: wg.at[2:4, k, c],
        lambda k: dev(z, x, k, c), wr_s, wr_r)
    swap = put(wg.at[:, :, c], wg.at[:, :, c], wc_s, wc_r, dev(z, x, y, 1 - c))
    swap_in = put(wg.at[:, :, 1 - c], wg.at[:, :, 1 - c], wc_s, wc_r, dev(z, x, y, 1 - c))
    far = (4, 3, 5, 2, 6, 1, 7)
    sent = [[put(parts[n].at[(z + k) % 8], gots[n].at[k - 1], z_s.at[n, k - 1], z_r.at[n, k - 1],
                 dev((z + k) % 8, x, y, c)) for k in far] for n in range(2)]
    blocks = [(x + k) % 4 for k in (0, 3, 1, 2)]

    def gather_y(n):
        g = gs[n]
        return ring(y, lambda k: g.at[x, k, c], lambda k: g.at[x, k, c, 0:32],
                    lambda k: g.at[x, k, c, 32:64], lambda k: dev(z, x, k, c),
                    gy_s.at[n], gy_r.at[n])

    def gather_x(n):
        g = gs[n]
        return ring(x, lambda k: g.at[k, :, c], lambda k: g.at[k, 0:2, c],
                    lambda k: g.at[k, 2:4, c], lambda k: dev(z, k, y, c), gx_s.at[n], gx_r.at[n])

    ry, rx = [gather_y(n) for n in range(2)], [gather_x(n) for n in range(2)]
    swaps = [[put(gs[n].at[b, :, c], gs[n].at[b, :, c], gc_s.at[n, i], gc_r.at[n, i],
                  dev(z, x, y, 1 - c)) for i, b in enumerate(blocks)] for n in range(2)]
    swapped = [[put(gs[n].at[b, :, 1 - c], gs[n].at[b, :, 1 - c], gc_s.at[n, i], gc_r.at[n, i],
                    dev(z, x, y, 1 - c)) for i, b in enumerate(blocks)] for n in range(2)]

    def weights_x():
        for d in wx:
            d.start()
        local[0].wait()
        a_start()

    def weights_y():
        for d in wx_in:
            d.wait_recv()
        w_start()

    def weights_core():
        w_finish()
        swap.start()
        a_finish()

    def product():
        swap_in.wait_recv()
        for n, (width, k0) in enumerate(((256, 0), (128, 256))):
            rhs = jnp.concatenate([wg[:, :, :, :, k0:k0 + width],
                                   wg[:, :, :, :, 384 + k0:384 + k0 + width]],
                                  axis=-1).reshape(FEAT, 2 * width)
            for half in range(2):
                lhs = jnp.concatenate(
                    [ag[xb, assign_ref[half * 4 + j]] for j in range(4) for xb in range(4)], axis=0)
                prod = jnp.dot(lhs, rhs, preferred_element_type=jnp.float32)
                parts[n][half * 4:half * 4 + 4] = prod.astype(jnp.bfloat16).reshape(4, 64, 2 * width)
            for d in sent[n]:
                d.start()

    def reduce_z(n):
        total = parts[n][z].astype(jnp.float32)
        for k in range(1, 8):
            put(parts[n].at[0], gots[n].at[k - 1], z_s.at[n, k - 1], z_r.at[n, k - 1],
                dev((z + 8 - k) % 8, x, y, c)).wait_recv()
            total = total + gots[n][k - 1].astype(jnp.float32)
        gs[n][x, y, c] = total.astype(jnp.bfloat16)
        ry[n][0]()

    def pairs_x(n):
        ry[n][2]()
        rx[n][0]()
        swaps[n][0].start()

    def pairs_xf(n):
        rx[n][1]()
        swaps[n][1].start()
        swaps[n][2].start()

    def pairs_xl(n):
        rx[n][2]()
        swaps[n][3].start()

    def cross_block(n, i):
        swapped[n][i].wait_recv()
        cross(blocks[i], n)

    def take(half):
        all_of(mvs[half], ex_s, ex_r, half).wait_recv()
        local[3 + half].wait()
        temporal(half)

    def finish(half):
        all_of(rts[half], rt_s, rt_r, half).wait_recv()
        back = rts[half][...].reshape(256, HALF).astype(jnp.float32)
        out_ref[:, cols[half]] = (acc[:, cols[half]] + back).astype(jnp.bfloat16)

    weights_x()
    exchange(0, 1, 8)
    weights_y()
    exchange(0, 8, 16)
    local[1].wait()
    local[2].wait()
    spatial(0, 2)
    a_forward()
    w_forward()
    exchange(0, 16, 32)
    spatial(2, 6)
    weights_core()
    product()
    exchange(1, 8, 24)
    take(0)
    reduce_z(0)
    reduce_z(1)
    exchange(1, 24, 32)
    ry[0][1]()
    ry[1][1]()
    pairs_x(0)
    exchange(1, 1, 8)
    local[5].wait()
    cross_block(0, 0)
    pairs_x(1)
    cross_block(1, 0)
    pairs_xf(0)
    give_back(0)
    cross_block(0, 1)
    cross_block(0, 2)
    pairs_xf(1)
    take(1)
    give_back(1)
    cross_block(1, 1)
    cross_block(1, 2)
    pairs_xl(0)
    cross_block(0, 3)
    pairs_xl(1)
    cross_block(1, 3)
    finish(0)
    finish(1)

    for half in range(2):
        all_of(mvs[half], ex_s, ex_r, half).wait_send()
        all_of(ts[half], rt_s, rt_r, half).wait_send()
    for d in wx + [swap] + sent[0] + sent[1] + swaps[0] + swaps[1]:
        d.wait_send()
    for drain in (a_drain, w_drain, ry[0][3], ry[1][3], rx[0][3], rx[1][3]):
        drain()


def body(latent_qkv, cross_query, residual, prompt_states, kv_weight, prompt_lengths, assignment):
    latent = jnp.transpose(latent_qkv[0, 0], (1, 0, 2)).reshape(3, 32, 8, 1536)
    sem = pltpu.SemaphoreType.DMA
    vm = pl.BlockSpec(memory_space=pltpu.VMEM)
    sm = pl.BlockSpec(memory_space=pltpu.SMEM)
    hb = pl.BlockSpec(memory_space=pltpu.MemorySpace.HBM)
    b16, f32 = jnp.bfloat16, jnp.float32
    out = pl.pallas_call(
        block_kernel,
        out_shape=jax.ShapeDtypeStruct((256, 1536), b16),
        in_specs=[sm, sm, hb, hb, hb, vm, vm],
        out_specs=vm,
        scratch_shapes=[
            pltpu.VMEM((4, ROWS, CB), b16),
            pltpu.VMEM((3, 32, 8, 1536), b16),
            pltpu.VMEM((256, 1536), b16),
            pltpu.VMEM((256, 1536), b16),
            pltpu.VMEM((256, 1536), f32),
            pltpu.VMEM((32, 3, 8, HALF), b16), pltpu.VMEM((32, 3, 8, HALF), b16),
            pltpu.VMEM((32, 8, HALF), b16), pltpu.VMEM((32, 8, HALF), b16),
            pltpu.VMEM((32, 8, HALF), b16), pltpu.VMEM((32, 8, HALF), b16),
            pltpu.VMEM((4, 8, ROWS, FEAT), b16),
            pltpu.VMEM((4, 4, 2, ROWS, CB), b16),
            pltpu.VMEM((8, 64, 512), b16), pltpu.VMEM((8, 64, 256), b16),
            pltpu.VMEM((7, 64, 512), b16), pltpu.VMEM((7, 64, 256), b16),
            pltpu.VMEM((4, 4, 2, 64, 512), b16), pltpu.VMEM((4, 4, 2, 64, 256), b16),
            sem((7,)), sem((2,)), sem((2,)), sem((2,)), sem((2,)),
            sem((3,)), sem((3,)), sem((4,)), sem((4,)), sem((4,)), sem((4,)),
            sem, sem, sem((2, 7)), sem((2, 7)),
            sem((2, 4)), sem((2, 4)), sem((2, 4)), sem((2, 4)), sem((2, 4)), sem((2, 4)),
        ],
        compiler_params=pltpu.CompilerParams(
            collective_id=0, has_side_effects=True),
        name="block",
    )(assignment, prompt_lengths, latent, cross_query[0, 0], residual[0, 0], prompt_states, kv_weight)
    return out[None, None]


def solution(mesh):
    return jax.shard_map(
        body,
        mesh=mesh,
        in_specs=(
            P("grp", "seq", None, None, "hd"),
            P("grp", "seq", None, "hd"),
            P("grp", "seq", None, "hd"),
            P(None, "seq", "grp"),
            P(("grp", "seq"), None, "hd"),
            P(),
            P(),
        ),
        out_specs=P("grp", "seq", None, "hd"),
        check_vma=False,
    )
```

```python
import math

import jax
import jax.numpy as jnp
from jax import lax
from jax.experimental import pallas as pl
from jax.experimental.pallas import tpu as pltpu
from jax.sharding import PartitionSpec as P

HDIM = 128
SCALE = 1.0 / math.sqrt(HDIM)
MESH = pl.DeviceIdType.MESH
ROWS, FEAT, CB, HALF = 16, 512, 768, 768


def soft(scores):
    top = jnp.max(scores, axis=-1, keepdims=True)
    powered = jnp.exp(scores - top)
    return (powered * (1.0 / jnp.sum(powered, axis=-1, keepdims=True))).astype(jnp.bfloat16)


def qk(q, k):
    return lax.dot_general(q, k, (((1,), (1,)), ((), ())), preferred_element_type=jnp.float32) * SCALE


def lanes(i):
    return pl.ds(pl.multiple_of(i * HDIM, HDIM), HDIM)


def block_kernel(assign_ref, len_ref, lat_ref, cq_ref, res_ref, a_ref, raw_ref, out_ref,
                 w_ref, lat, cq, res, acc, mv0, mv1, t0, t1, rt0, rt1, ag, wg, part0, part1, got0, got1, g0, g1,
                 loc, ex_s, ex_r, rt_s, rt_r,
                 wx_s, wx_r, ar_s, ar_r, wr_s, wr_r, wc_s, wc_r, z_s, z_r,
                 gy_s, gy_r, gx_s, gx_r, gc_s, gc_r):
    z = lax.axis_index("grp")
    s = lax.axis_index("seq")
    h = lax.axis_index("hd")
    x = s // 8
    y = (s // 2) % 4
    c = s % 2

    def dev(zz, xx, yy, cc):
        return (zz, (xx * 4 + yy) * 2 + cc, h)

    def put(src, dst, ss, rs, to):
        return pltpu.make_async_remote_copy(
            src_ref=src, dst_ref=dst, send_sem=ss, recv_sem=rs,
            device_id=to, device_id_type=MESH)

    def peer(t):
        return (((x + t // 8) % 4) * 4 + (y + t) % 4) * 2 + (c + t // 4) % 2

    mvs, ts, rts = (mv0, mv1), (t0, t1), (rt0, rt1)
    cols = (pl.ds(0, HALF), pl.ds(HALF, HALF))
    local = [
        pltpu.make_async_copy(a_ref, ag.at[x], loc.at[1]),
        pltpu.make_async_copy(lat_ref, lat, loc.at[2]),
        pltpu.make_async_copy(res_ref, res, loc.at[3]),
        pltpu.make_async_copy(lat_ref.at[:, s, :, cols[0]], mv0.at[s], loc.at[4]),
        pltpu.make_async_copy(lat_ref.at[:, s, :, cols[1]], mv1.at[s], loc.at[5]),
        pltpu.make_async_copy(cq_ref, cq, loc.at[6]),
    ]
    for d in local:
        d.start()

    barrier = pltpu.get_barrier_semaphore()

    @pl.loop(1, 32)
    def _(t):
        pl.semaphore_signal(barrier, inc=1, device_id=(z, peer(t), h), device_id_type=MESH)

    @pl.loop(1, 8)
    def _(k):
        pl.semaphore_signal(barrier, inc=1, device_id=((z + k) % 8, s, h), device_id_type=MESH)

    for n in range(2):
        rows = raw_ref[:, n, :]
        for k in range(4):
            w_ref[k, :, n * 384:(n + 1) * 384] = rows[:, k * 384:(k + 1) * 384]
    wg[x, y, c] = w_ref[x]
    pl.semaphore_wait(barrier, 38)

    def ring(me, at, lo, hi, to, ss, rs):
        left, right = (me + 3) % 4, (me + 1) % 4
        opp = (me + 2) % 4
        first = [put(at(me), at(me), ss.at[0], rs.at[0], to(right)),
                 put(at(me), at(me), ss.at[1], rs.at[1], to(left))]
        second = [put(lo(left), lo(left), ss.at[2], rs.at[2], to(right)),
                  put(hi(right), hi(right), ss.at[3], rs.at[3], to(left))]
        arrive = [put(at(left), at(left), ss.at[0], rs.at[0], to(right)),
                  put(at(right), at(right), ss.at[1], rs.at[1], to(left)),
                  put(lo(opp), lo(opp), ss.at[2], rs.at[2], to(right)),
                  put(hi(opp), hi(opp), ss.at[3], rs.at[3], to(left))]

        def start():
            first[0].start()
            first[1].start()

        def forward():
            arrive[0].wait_recv()
            second[0].start()
            arrive[1].wait_recv()
            second[1].start()

        def finish():
            arrive[2].wait_recv()
            arrive[3].wait_recv()

        def drain():
            for d in first + second:
                d.wait_send()

        return start, forward, finish, drain

    def exchange(half, lo, hi):
        @pl.loop(lo, hi)
        def _(t):
            to = peer(t)
            put(lat_ref.at[:, to, :, cols[half]], mvs[half].at[s],
                ex_s.at[half], ex_r.at[half], (z, to, h)).start()

    def give_back(half, lo=1, hi=32):
        @pl.loop(lo, hi)
        def _(t):
            to = peer(t)
            put(ts[half].at[to], rts[half].at[s], rt_s.at[half], rt_r.at[half], (z, to, h)).start()

    def all_of(ref, ss, rs, half):
        whole = ref.at[pl.ds(0, 31)]
        return put(whole, whole, ss.at[half], rs.at[half], (z, peer(1), h))

    def spatial(lo, hi):
        @pl.loop(lo, hi)
        def _(i):
            for j in range(2):
                at = lanes(i * 2 + j)
                q, k, v = (lat[n, :, :, at].reshape(256, HDIM) for n in range(3))
                o = jnp.dot(soft(qk(q, k)), v, preferred_element_type=jnp.float32)
                acc[:, at] = res[:, at].astype(jnp.float32) + o

    def temporal(half):
        mv, t = mvs[half], ts[half]
        row = lax.broadcasted_iota(jnp.int32, (256, 256), 0) % 8
        col = lax.broadcasted_iota(jnp.int32, (256, 256), 1) % 8

        @pl.loop(0, 3)
        def _(i):
            for j in range(2):
                at = lanes(i * 2 + j)
                q, k, v = (mv[:, n, :, at].reshape(256, HDIM) for n in range(3))
                w = soft(jnp.where(row == col, qk(q, k), -1e30))
                o = jnp.dot(w, v, preferred_element_type=jnp.float32)
                t[:, :, at] = o.astype(jnp.bfloat16).reshape(32, 8, HDIM)

        rts[half][pl.ds(s, 1)] = t[pl.ds(s, 1)]

    r = lax.broadcasted_iota(jnp.int32, (1, 512), 1)
    pos = ((((r // 16) % 4) * 4 + r // 128) * 2 + (r // 64) % 2) * 16 + r % 16
    bias = jnp.where(pos < len_ref[assign_ref[z]], 0.0, -1e9)

    parts, gots, gs = (part0, part1), (got0, got1), (g0, g1)
    group_heads = ((0, 1), (2,))

    def cross(b, n):
        heads = group_heads[n]
        for j, head in enumerate(heads):
            at = lanes(b * 3 + head)
            vj = len(heads) + j
            k = gs[n][b, :, :, :, j * HDIM:(j + 1) * HDIM].reshape(512, HDIM)
            v = gs[n][b, :, :, :, vj * HDIM:(vj + 1) * HDIM].reshape(512, HDIM)
            w = soft(qk(cq[:, at], k) + bias)
            acc[:, at] = acc[:, at] + jnp.dot(w, v, preferred_element_type=jnp.float32)

    wx = [put(w_ref.at[(x + k) % 4], wg.at[x, y, c], wx_s.at[k - 1], wx_r.at[k - 1],
              dev(z, (x + k) % 4, y, c)) for k in (1, 2, 3)]
    wx_in = [put(w_ref.at[x], wg.at[(x + 4 - k) % 4, y, c], wx_s.at[k - 1], wx_r.at[k - 1],
                 dev(z, (x + 4 - k) % 4, y, c)) for k in (1, 2, 3)]
    a_start, a_forward, a_finish, a_drain = ring(
        x, lambda k: ag.at[k], lambda k: ag.at[k, 0:4], lambda k: ag.at[k, 4:8],
        lambda k: dev(z, k, y, c), ar_s, ar_r)
    w_start, w_forward, w_finish, w_drain = ring(
        y, lambda k: wg.at[:, k, c], lambda k: wg.at[0:2, k, c], lambda k: wg.at[2:4, k, c],
        lambda k: dev(z, x, k, c), wr_s, wr_r)
    swap = put(wg.at[:, :, c], wg.at[:, :, c], wc_s, wc_r, dev(z, x, y, 1 - c))
    swap_in = put(wg.at[:, :, 1 - c], wg.at[:, :, 1 - c], wc_s, wc_r, dev(z, x, y, 1 - c))
    far = (4, 3, 5, 2, 6, 1, 7)
    sent = [[put(parts[n].at[(z + k) % 8], gots[n].at[k - 1], z_s.at[n, k - 1], z_r.at[n, k - 1],
                 dev((z + k) % 8, x, y, c)) for k in far] for n in range(2)]
    blocks = [(x + k) % 4 for k in (0, 3, 1, 2)]

    def gather_y(n):
        g = gs[n]
        return ring(y, lambda k: g.at[x, k, c], lambda k: g.at[x, k, c, 0:32],
                    lambda k: g.at[x, k, c, 32:64], lambda k: dev(z, x, k, c),
                    gy_s.at[n], gy_r.at[n])

    def gather_x(n):
        g = gs[n]
        return ring(x, lambda k: g.at[k, :, c], lambda k: g.at[k, 0:2, c],
                    lambda k: g.at[k, 2:4, c], lambda k: dev(z, k, y, c), gx_s.at[n], gx_r.at[n])

    ry, rx = [gather_y(n) for n in range(2)], [gather_x(n) for n in range(2)]
    swaps = [[put(gs[n].at[b, :, c], gs[n].at[b, :, c], gc_s.at[n, i], gc_r.at[n, i],
                  dev(z, x, y, 1 - c)) for i, b in enumerate(blocks)] for n in range(2)]
    swapped = [[put(gs[n].at[b, :, 1 - c], gs[n].at[b, :, 1 - c], gc_s.at[n, i], gc_r.at[n, i],
                    dev(z, x, y, 1 - c)) for i, b in enumerate(blocks)] for n in range(2)]

    def weights_x():
        for d in wx:
            d.start()
        local[0].wait()
        a_start()

    def weights_y():
        for d in wx_in:
            d.wait_recv()
        w_start()

    def weights_core():
        w_finish()
        swap.start()
        a_finish()

    def product():
        swap_in.wait_recv()
        for n, (width, k0) in enumerate(((256, 0), (128, 256))):
            rhs = jnp.concatenate([wg[:, :, :, :, k0:k0 + width],
                                   wg[:, :, :, :, 384 + k0:384 + k0 + width]],
                                  axis=-1).reshape(FEAT, 2 * width)
            for half in range(2):
                lhs = jnp.concatenate(
                    [ag[xb, assign_ref[half * 4 + j]] for j in range(4) for xb in range(4)], axis=0)
                prod = jnp.dot(lhs, rhs, preferred_element_type=jnp.float32)
                parts[n][half * 4:half * 4 + 4] = prod.astype(jnp.bfloat16).reshape(4, 64, 2 * width)
            for d in sent[n]:
                d.start()

    def reduce_z(n):
        total = parts[n][z].astype(jnp.float32)
        for k in range(1, 8):
            put(parts[n].at[0], gots[n].at[k - 1], z_s.at[n, k - 1], z_r.at[n, k - 1],
                dev((z + 8 - k) % 8, x, y, c)).wait_recv()
            total = total + gots[n][k - 1].astype(jnp.float32)
        gs[n][x, y, c] = total.astype(jnp.bfloat16)
        ry[n][0]()

    def pairs_x(n):
        ry[n][2]()
        rx[n][0]()
        swaps[n][0].start()

    def pairs_xf(n):
        rx[n][1]()
        swaps[n][1].start()
        swaps[n][2].start()

    def pairs_xl(n):
        rx[n][2]()
        swaps[n][3].start()

    def cross_block(n, i):
        swapped[n][i].wait_recv()
        cross(blocks[i], n)

    def take(half):
        all_of(mvs[half], ex_s, ex_r, half).wait_recv()
        local[3 + half].wait()
        temporal(half)

    def finish(half):
        all_of(rts[half], rt_s, rt_r, half).wait_recv()
        back = rts[half][...].reshape(256, HALF).astype(jnp.float32)
        out_ref[:, cols[half]] = (acc[:, cols[half]] + back).astype(jnp.bfloat16)

    weights_x()
    exchange(0, 1, 4)
    weights_y()
    exchange(0, 4, 12)
    local[1].wait()
    local[2].wait()
    spatial(0, 2)
    a_forward()
    w_forward()
    exchange(0, 12, 32)
    spatial(2, 6)
    weights_core()
    product()
    exchange(1, 8, 24)
    take(0)
    reduce_z(0)
    reduce_z(1)
    exchange(1, 24, 32)
    ry[0][1]()
    ry[1][1]()
    pairs_x(0)
    exchange(1, 1, 8)
    local[5].wait()
    cross_block(0, 0)
    pairs_x(1)
    cross_block(1, 0)
    give_back(0, 1, 8)
    pairs_xf(0)
    give_back(0, 8, 32)
    cross_block(0, 1)
    cross_block(0, 2)
    pairs_xf(1)
    take(1)
    give_back(1)
    cross_block(1, 1)
    cross_block(1, 2)
    pairs_xl(0)
    cross_block(0, 3)
    pairs_xl(1)
    cross_block(1, 3)
    finish(0)
    finish(1)

    for half in range(2):
        all_of(mvs[half], ex_s, ex_r, half).wait_send()
        all_of(ts[half], rt_s, rt_r, half).wait_send()
    for d in wx + [swap] + sent[0] + sent[1] + swaps[0] + swaps[1]:
        d.wait_send()
    for drain in (a_drain, w_drain, ry[0][3], ry[1][3], rx[0][3], rx[1][3]):
        drain()


def body(latent_qkv, cross_query, residual, prompt_states, kv_weight, prompt_lengths, assignment):
    latent = jnp.transpose(latent_qkv[0, 0], (1, 0, 2)).reshape(3, 32, 8, 1536)
    sem = pltpu.SemaphoreType.DMA
    vm = pl.BlockSpec(memory_space=pltpu.VMEM)
    sm = pl.BlockSpec(memory_space=pltpu.SMEM)
    hb = pl.BlockSpec(memory_space=pltpu.MemorySpace.HBM)
    b16, f32 = jnp.bfloat16, jnp.float32
    out = pl.pallas_call(
        block_kernel,
        out_shape=jax.ShapeDtypeStruct((256, 1536), b16),
        in_specs=[sm, sm, hb, hb, hb, vm, vm],
        out_specs=vm,
        scratch_shapes=[
            pltpu.VMEM((4, ROWS, CB), b16),
            pltpu.VMEM((3, 32, 8, 1536), b16),
            pltpu.VMEM((256, 1536), b16),
            pltpu.VMEM((256, 1536), b16),
            pltpu.VMEM((256, 1536), f32),
            pltpu.VMEM((32, 3, 8, HALF), b16), pltpu.VMEM((32, 3, 8, HALF), b16),
            pltpu.VMEM((32, 8, HALF), b16), pltpu.VMEM((32, 8, HALF), b16),
            pltpu.VMEM((32, 8, HALF), b16), pltpu.VMEM((32, 8, HALF), b16),
            pltpu.VMEM((4, 8, ROWS, FEAT), b16),
            pltpu.VMEM((4, 4, 2, ROWS, CB), b16),
            pltpu.VMEM((8, 64, 512), b16), pltpu.VMEM((8, 64, 256), b16),
            pltpu.VMEM((7, 64, 512), b16), pltpu.VMEM((7, 64, 256), b16),
            pltpu.VMEM((4, 4, 2, 64, 512), b16), pltpu.VMEM((4, 4, 2, 64, 256), b16),
            sem((7,)), sem((2,)), sem((2,)), sem((2,)), sem((2,)),
            sem((3,)), sem((3,)), sem((4,)), sem((4,)), sem((4,)), sem((4,)),
            sem, sem, sem((2, 7)), sem((2, 7)),
            sem((2, 4)), sem((2, 4)), sem((2, 4)), sem((2, 4)), sem((2, 4)), sem((2, 4)),
        ],
        compiler_params=pltpu.CompilerParams(
            collective_id=0, has_side_effects=True),
        name="block",
    )(assignment, prompt_lengths, latent, cross_query[0, 0], residual[0, 0], prompt_states, kv_weight)
    return out[None, None]


def solution(mesh):
    return jax.shard_map(
        body,
        mesh=mesh,
        in_specs=(
            P("grp", "seq", None, None, "hd"),
            P("grp", "seq", None, "hd"),
            P("grp", "seq", None, "hd"),
            P(None, "seq", "grp"),
            P(("grp", "seq"), None, "hd"),
            P(),
            P(),
        ),
        out_specs=P("grp", "seq", None, "hd"),
        check_vma=False,
    )
```
